256 devices in a mesh: row: 16 (over z, core), col: 16 (over x, y).
Axes of the slice: x: 4, y: 4, z: 8, core: 2. Of those that a mesh axis runs over, the one named last changes fastest.
Arguments:
- hamiltonian: bfloat16 [36864, 36864], P('row', 'col'), may hold values from -0.6 to 0.6, as said below
- start_vectors: float32 [8, 16, 2304], P(None, 'col', 'row'), may hold values from -20 to 20
Outputs:
- last_vectors: float32 [8, 36864], P(None, ('row', 'col'))
- moments: float32 [8, 4], replicated
The draws below stay inside these ranges and needn't reach their ends.
Inputs may be any that keep to these rules, and one draw needn't show every extreme that they name: `hamiltonian`: the matrix is exactly symmetric.
All inputs are finite; a program needn't handle non-finite values.
Results may differ from the reference program's by a relative error of at most 0.0024.
Values may be sent and summed in bfloat16 or wider, within the bound.
A program may use at most 64 MiB of HBM per device.

```python
import math
import jax
import jax.numpy as jnp
from jax import lax

NVEC = 8
STEPS = 3
ORDER = 36864
BLOCK_C = 2304


def draw_hamiltonian(key, part):
    tile_count = 16
    tile_width = ORDER // tile_count
    spread = 0.12 / math.sqrt(ORDER)
    offsets = jax.random.uniform(jax.random.fold_in(key, 7), (ORDER,), jnp.float32, -0.55, 0.55)
    base_key = jax.random.fold_in(key, 11)

    def random_tile(tile_number):
        tile_key = jax.random.fold_in(base_key, tile_number)
        values = jnp.clip(jax.random.normal(tile_key, (tile_width, tile_width), jnp.float32), -6.0, 6.0)
        return values * spread

    def row_strip(upper_index):

        def paired(other_index):
            return random_tile(upper_index * tile_count + other_index) + random_tile(other_index * tile_count + upper_index).T
        tiles = jax.vmap(paired)(jnp.arange(tile_count, dtype=jnp.int32))
        strip = jnp.moveaxis(tiles, 0, 1).reshape(tile_width, ORDER)
        diag_part = lax.dynamic_slice_in_dim(offsets, upper_index * tile_width, tile_width)
        rows_here = upper_index * tile_width + jnp.arange(tile_width, dtype=jnp.int32)
        on_diagonal = jnp.arange(ORDER, dtype=jnp.int32)[None, :] == rows_here[:, None]
        strip = strip + jnp.where(on_diagonal, diag_part[:, None], 0.0)
        return strip.astype(jnp.bfloat16)
    strips = lax.map(row_strip, jnp.arange(tile_count, dtype=jnp.int32))
    return strips.reshape(ORDER, ORDER)


def draw_start_vectors(key, part):
    ramp = jnp.arange(ORDER, dtype=jnp.float32) / ORDER
    scales = 10.0 ** (ramp - 0.5)
    values = scales[None, :] * jnp.clip(jax.random.normal(key, (NVEC, ORDER), jnp.float32), -6.0, 6.0)
    return values.reshape(NVEC, ORDER // BLOCK_C, BLOCK_C).astype(jnp.float32)


def setup_inputs(seed: int = 0) -> dict:
    seeds = jax.random.split(jax.random.key(seed), 3)
    return {
        "hamiltonian": draw_hamiltonian(jax.random.fold_in(seeds[2], 71), 0),
        "start_vectors": draw_start_vectors(jax.random.fold_in(seeds[2], 71), 0),
    }


def reference(hamiltonian, start_vectors):
    current = start_vectors.reshape(start_vectors.shape[0], -1)
    previous = current
    squares = [jnp.sum(current * current, axis=1) / ORDER]
    for level in range(STEPS):
        narrow = current.astype(jnp.bfloat16)
        applied = jnp.dot(narrow, hamiltonian, preferred_element_type=jnp.float32)
        if level == 0:
            following = applied
        else:
            following = 2.0 * applied - previous
        previous = current
        current = following
        squares.append(jnp.sum(current * current, axis=1) / ORDER)
    stacked = jnp.stack(squares, axis=1)
    moments = jnp.concatenate([stacked[:, :1], 2.0 * stacked[:, 1:] - stacked[:, :1]], axis=1)
    return current, moments
```

```python
import functools

import jax
import jax.numpy as jnp
from jax import lax
from jax.experimental import pallas as pl
from jax.experimental.pallas import tpu as pltpu
from jax.sharding import PartitionSpec as P

ORDER = 36864
NVEC = 8
GROUP = 16
PIECE = 144
TILE = 256
TILES = 9
BLOCK = TILE * TILES
F32 = jnp.float32
BF16 = jnp.bfloat16


def row_home(tile):
    return jnp.where(tile == TILES - 1, 8, 2 * tile + 1)


def col_home(tile, parity):
    return jnp.where(parity == 0, tile, GROUP - 1 - tile)


def kernel(
    h_ref, v_ref, last_ref, mom_ref,
    h, p0_own, p0, v0_own, v0_in, x0, v1_keep,
    part1, in1, ag1_own, ag1, part2, in2, ag2_own, ag2, part3, in3,
    out_own, out_in, sq, m1_own, m1, m2_own, m2,
    h_sem, p0_s, p0_r, v0_s, v0_r, rs_s, rs_r, ag_s, ag_r, out_s, out_r, m_s, m_r,
):
    row, col = lax.axis_index("row"), lax.axis_index("col")
    parity = lax.rem(row, 2)

    chip = row // 2
    row_red = (parity == 1) | (row == 8)
    row_tile = jnp.where(row == 8, TILES - 1, chip)
    col_slot = jnp.where(parity == 0, col, GROUP - 1 - col)
    col_red = col_slot < TILES
    col_tile = jnp.where(col_red, col_slot, col_slot - 7)

    def peer(axis, index):
        return (index, col) if axis == "row" else (row, index)

    def send(src, dst, s_sem, r_sem, axis, index):
        pltpu.make_async_remote_copy(
            src_ref=src, dst_ref=dst, send_sem=s_sem, recv_sem=r_sem,
            device_id=peer(axis, index), device_id_type=pl.DeviceIdType.MESH,
        ).start()

    def wait_for(ref, sem):
        pltpu.make_async_copy(ref, ref, sem).wait()

    def others(axis):
        me = row if axis == "row" else col
        return [lax.rem(me + k, GROUP) for k in (8, 7, 9, 6, 10, 5, 11, 4, 12, 3, 13, 2, 14, 1, 15)]

    def nth(first, i):
        return lax.rem(first + 1 + i, TILES)

    def h_rows(tile):
        return pl.ds(pl.multiple_of(tile * TILE, TILE), TILE)

    loads = []
    for i in range(TILES):
        rows = h_rows(nth(col_tile, i))
        loads.append(pltpu.make_async_copy(h_ref.at[rows, :], h.at[rows, :], h_sem.at[i]))
        loads[-1].start()

    barrier = pltpu.get_barrier_semaphore()
    for axis in ("row", "col"):
        for index in others(axis):
            pl.semaphore_signal(
                barrier, inc=1, device_id=peer(axis, index), device_id_type=pl.DeviceIdType.MESH
            )

    lane = lax.broadcasted_iota(jnp.int32, (NVEC, TILE), 1)
    start = jnp.concatenate(
        [v_ref[:, 0, :], jnp.zeros((NVEC, TILE - PIECE), F32)], axis=1
    )
    v0_own[...] = start
    p0_own[...] = start.astype(BF16)
    sq[0] = jnp.sum(start * start, axis=1, keepdims=True)
    for n in (1, 2, 3):
        sq[n] = jnp.zeros((NVEC, 1), F32)
    pl.semaphore_wait(barrier, 2 * (GROUP - 1))

    for index in others("row"):
        send(p0_own, p0.at[row], p0_s, p0_r, "row", index)
    p0[row] = start.astype(BF16)

    first_tile = (PIECE * row) // TILE
    last_tile = (PIECE * row + PIECE - 1) // TILE
    for n, tile in enumerate((first_tile, last_tile)):
        home = row_home(tile)
        slot = row - (TILE * tile) // PIECE
        wanted = jnp.bool_(True) if n == 0 else last_tile != first_tile

        @pl.when(wanted & (home != row))
        def _():
            send(v0_own, v0_in.at[slot], v0_s.at[n], v0_r.at[slot], "row", home)

        @pl.when(wanted & (home == row))
        def _():
            v0_in[slot] = start

    wait_for(p0.at[pl.ds(0, GROUP - 1)], p0_r)
    tiles = [jnp.zeros((NVEC, TILE), F32) for _ in range(TILES)]
    for j in range(GROUP):
        at, shift = divmod(PIECE * j, TILE)
        piece = p0[j].astype(F32)
        turned = pltpu.roll(piece, shift, axis=1) if shift else piece
        tiles[at] = jnp.where((lane >= shift) & (lane < shift + PIECE), turned, tiles[at])
        if shift + PIECE > TILE:
            tiles[at + 1] = jnp.where(lane < shift + PIECE - TILE, turned, tiles[at + 1])
    for k in range(TILES):
        x0[k] = tiles[k].astype(BF16)

    def multiply(x, turned, first, is_red, axis, part, arrived, n):
        me = row if axis == "row" else col
        narrow = jnp.concatenate([x[k] for k in range(TILES)], axis=1)
        for i in range(TILES):
            tile = nth(first, i)
            if n == 0:
                loads[i].wait()
            if turned:
                block = h[h_rows(tile), :]
                value = lax.dot_general(
                    narrow, block, (((1,), (1,)), ((), ())), preferred_element_type=F32
                )
            else:
                value = jnp.dot(narrow, h[:, h_rows(tile)], preferred_element_type=F32)
            home = row_home(tile) if axis == "row" else col_home(tile, parity)
            if i < TILES - 1:
                part[i] = value
                send(part.at[i], arrived.at[me], rs_s.at[n], rs_r.at[n], axis, home)
            else:

                @pl.when(is_red)
                def _():
                    arrived[me] = value

                @pl.when(jnp.logical_not(is_red))
                def _():
                    part[i] = value
                    send(part.at[i], arrived.at[me], rs_s.at[n], rs_r.at[n], axis, home)

    def summed(arrived, n):
        wait_for(arrived.at[pl.ds(0, GROUP - 1)], rs_r.at[n])
        terms = [arrived[j] for j in range(GROUP)]
        while len(terms) > 1:
            terms = [terms[k] + terms[k + 1] for k in range(0, len(terms), 2)]
        return terms[0]

    def to_all(value, own, dest, tile, axis, n):
        own[...] = value.astype(BF16)
        for index in others(axis):
            send(own, dest.at[tile], ag_s.at[n], ag_r.at[n], axis, index)
        dest[tile] = value.astype(BF16)

    def gathered(dest, is_red, n):
        @pl.when(is_red)
        def _():
            wait_for(dest.at[pl.ds(0, TILES - 1)], ag_r.at[n])

        @pl.when(jnp.logical_not(is_red))
        def _():
            wait_for(dest, ag_r.at[n])

    def square(value):
        return jnp.sum(value * value, axis=1, keepdims=True)

    multiply(x0, True, col_tile, col_red, "col", part1, in1, 0)

    @pl.when(col_red)
    def _():
        v1 = summed(in1, 0)
        to_all(v1, ag1_own, ag1, col_tile, "col", 0)
        v1_keep[...] = v1
        sq[1] = square(v1)

    gathered(ag1, col_red, 0)

    multiply(ag1, False, row_tile, row_red, "row", part2, in2, 1)

    @pl.when(row_red)
    def _():
        v0 = jnp.zeros((NVEC, TILE), F32)
        for slot in range(3):
            owner = (TILE * row_tile) // PIECE + slot
            offset = PIECE * owner - TILE * row_tile

            @pl.when((offset < TILE) & (owner != row))
            def _():
                wait_for(v0_in.at[slot], v0_r.at[slot])

            turned = pltpu.roll(v0_in[slot], lax.rem(offset + TILE, TILE), axis=1)
            v0 = jnp.where((lane >= offset) & (lane < offset + PIECE), turned, v0)
        v2 = 2.0 * summed(in2, 1) - v0
        to_all(v2, ag2_own, ag2, row_tile, "row", 1)
        sq[2] = square(v2)

    gathered(ag2, row_red, 1)

    multiply(ag2, True, col_tile, col_red, "col", part3, in3, 2)

    def out_dest(slot):
        owner = (TILE * col_tile) // PIECE + slot
        return owner, PIECE * owner < TILE * (col_tile + 1), col_tile - (PIECE * owner) // TILE

    @pl.when(col_red)
    def _():
        v3 = 2.0 * summed(in3, 2) - v1_keep[...]
        out_own[...] = v3
        sq[3] = square(v3)

    wide = lax.broadcasted_iota(jnp.int32, (NVEC, 128), 1)
    sub = lax.broadcasted_iota(jnp.int32, (NVEC, 128), 0)
    packed = jnp.zeros((NVEC, 128), F32)
    for n in range(4):
        packed = jnp.where(wide == 4 * sub + n, sq[n], packed)

    def everywhere(value, own, dest, axis, n):
        me = row if axis == "row" else col
        own[...] = value
        for index in others(axis):
            send(own, dest.at[me], m_s.at[n], m_r.at[n], axis, index)
        dest[me] = value

    def total(dest, n):
        wait_for(dest.at[pl.ds(0, GROUP - 1)], m_r.at[n])
        terms = [dest[j] for j in range(GROUP)]
        while len(terms) > 1:
            terms = [terms[k] + terms[k + 1] for k in range(0, len(terms), 2)]
        return terms[0]

    everywhere(jnp.sum(packed, axis=0, keepdims=True), m1_own, m1, "col", 0)

    for slot in range(3):
        owner, wanted, place = out_dest(slot)

        @pl.when(col_red & wanted & (owner != col))
        def _():
            send(out_own, out_in.at[place], out_s.at[slot], out_r.at[place], "col", owner)

        @pl.when(col_red & wanted & (owner == col))
        def _():
            out_in[place] = out_own[...]

    everywhere(total(m1, 0), m2_own, m2, "row", 1)

    from_tile = (PIECE * col) // TILE
    upto_tile = (PIECE * col + PIECE - 1) // TILE

    @pl.when(col_home(from_tile, parity) != col)
    def _():
        wait_for(out_in.at[0], out_r.at[0])

    @pl.when((upto_tile != from_tile) & (col_home(upto_tile, parity) != col))
    def _():
        wait_for(out_in.at[1], out_r.at[1])

    both = jnp.concatenate([out_in[0], out_in[1]], axis=1)
    begin = PIECE * col - TILE * from_tile
    last_ref[...] = pltpu.roll(both, lax.rem(2 * TILE - begin, 2 * TILE), axis=1)[:, :PIECE]

    wait_for(p0.at[pl.ds(0, GROUP - 1)], p0_s)
    for n, tile in enumerate((first_tile, last_tile)):
        wanted = jnp.bool_(True) if n == 0 else last_tile != first_tile

        @pl.when(wanted & (row_home(tile) != row))
        def _():
            wait_for(v0_own, v0_s.at[n])

    for n, (part, is_red) in enumerate(((part1, col_red), (part2, row_red), (part3, col_red))):

        @pl.when(is_red)
        def _():
            wait_for(part.at[pl.ds(0, TILES - 1)], rs_s.at[n])

        @pl.when(jnp.logical_not(is_red))
        def _():
            wait_for(part, rs_s.at[n])

    for n, is_red in enumerate((col_red, row_red)):

        @pl.when(is_red)
        def _():
            wait_for(p0.at[pl.ds(0, GROUP - 1)], ag_s.at[n])

    for slot in range(3):
        owner, wanted, _place = out_dest(slot)

        @pl.when(col_red & wanted & (owner != col))
        def _():
            wait_for(out_own, out_s.at[slot])

    wait_for(m1.at[pl.ds(0, GROUP - 1)], m_s.at[0])

    squares = total(m2, 1) / ORDER
    spread = jnp.broadcast_to(squares, (NVEC, 128))
    by_order = [
        jnp.sum(jnp.where(wide == 4 * sub + n, spread, 0.0), axis=1, keepdims=True)
        for n in range(4)
    ]
    mom_ref[...] = jnp.concatenate(
        [by_order[0]] + [2.0 * by_order[n] - by_order[0] for n in (1, 2, 3)], axis=1
    )
    wait_for(m2.at[pl.ds(0, GROUP - 1)], m_s.at[1])


def per_device(hamiltonian, start_vectors):
    dma = pltpu.SemaphoreType.DMA
    rowed = pltpu.VMEM((GROUP, 1, 128), F32)
    tile = pltpu.VMEM((NVEC, TILE), F32)
    narrow = pltpu.VMEM((NVEC, TILE), BF16)
    return pl.pallas_call(
        kernel,
        out_shape=(
            jax.ShapeDtypeStruct((NVEC, PIECE), F32),
            jax.ShapeDtypeStruct((NVEC, 4), F32),
        ),
        in_specs=[
            pl.BlockSpec(memory_space=pl.ANY),
            pl.BlockSpec(memory_space=pltpu.VMEM),
        ],
        out_specs=(
            pl.BlockSpec(memory_space=pltpu.VMEM),
            pl.BlockSpec(memory_space=pltpu.VMEM),
        ),
        scratch_shapes=[
            pltpu.VMEM((BLOCK, BLOCK), BF16),
            narrow, pltpu.VMEM((GROUP, NVEC, TILE), BF16),
            tile, pltpu.VMEM((3, NVEC, TILE), F32),
            pltpu.VMEM((TILES, NVEC, TILE), BF16), tile,
            pltpu.VMEM((TILES, NVEC, TILE), F32), pltpu.VMEM((GROUP, NVEC, TILE), F32),
            narrow, pltpu.VMEM((TILES, NVEC, TILE), BF16),
            pltpu.VMEM((TILES, NVEC, TILE), F32), pltpu.VMEM((GROUP, NVEC, TILE), F32),
            narrow, pltpu.VMEM((TILES, NVEC, TILE), BF16),
            pltpu.VMEM((TILES, NVEC, TILE), F32), pltpu.VMEM((GROUP, NVEC, TILE), F32),
            tile, pltpu.VMEM((2, NVEC, TILE), F32),
            pltpu.VMEM((4, NVEC, 1), F32),
            pltpu.VMEM((1, 128), F32), rowed, pltpu.VMEM((1, 128), F32), rowed,
            dma((TILES,)), dma(()), dma(()), dma((2,)), dma((3,)), dma((3,)), dma((3,)),
            dma((2,)), dma((2,)), dma((3,)), dma((2,)), dma((2,)), dma((2,)),
        ],
        compiler_params=pltpu.CompilerParams(
            collective_id=0, has_side_effects=True, vmem_limit_bytes=60 * 1024 * 1024
        ),
    )(hamiltonian, start_vectors)


def solution(mesh):
    return jax.shard_map(
        per_device,
        mesh=mesh,
        in_specs=(P("row", "col"), P(None, "col", "row")),
        out_specs=(P(None, ("row", "col")), P()),
        check_vma=False,
    )
```

```python
import functools

import jax
import jax.numpy as jnp
from jax import lax
from jax.experimental import pallas as pl
from jax.experimental.pallas import tpu as pltpu
from jax.sharding import PartitionSpec as P

ORDER = 36864
NVEC = 8
GROUP = 16
PIECE = 144
TILE = 256
TILES = 9
BLOCK = TILE * TILES
F32 = jnp.float32
BF16 = jnp.bfloat16


def row_home(tile):
    return jnp.where(tile == TILES - 1, 8, 2 * tile + 1)


def col_home(tile, parity):
    return jnp.where(parity == 0, tile, GROUP - 1 - tile)


def kernel(
    h_ref, v_ref, last_ref, mom_ref,
    v_own, h, h_t, p0_own, p0, v0_own, v0_in, x0, v1_keep,
    part1, in1, ag1_own, ag1, part2, in2, ag2_own, ag2, part3, in3,
    out_own, out_in, sq, m1_own, m1, m2_own, m2,
    v_sem, h_sem, p0_s, p0_r, v0_s, v0_r, rs_s, rs_r, ag_s, ag_r, out_s, out_r, m_s, m_r,
):
    row, col = lax.axis_index("row"), lax.axis_index("col")
    parity = lax.rem(row, 2)

    chip = row // 2
    row_red = (parity == 1) | (row == 8)
    row_tile = jnp.where(row == 8, TILES - 1, chip)
    col_tiles = (col, GROUP - 1 - col)
    col_reds = tuple((parity == 1) & (tile < TILES) for tile in col_tiles)
    col_red = col_reds[1]
    col_slot = jnp.where(parity == 0, col, GROUP - 1 - col)
    col_tile = jnp.where(col_slot < TILES, col_slot, col_slot - 7)
    odd_row = row + 1 - parity
    mate_row = row + 1 - 2 * parity

    def peer(axis, index):
        return (index, col) if axis == "row" else (row, index)

    def send_to(src, dst, s_sem, r_sem, device):
        pltpu.make_async_remote_copy(
            src_ref=src, dst_ref=dst, send_sem=s_sem, recv_sem=r_sem,
            device_id=device, device_id_type=pl.DeviceIdType.MESH,
        ).start()

    def send(src, dst, s_sem, r_sem, axis, index):
        send_to(src, dst, s_sem, r_sem, peer(axis, index))

    def wait_for(ref, sem):
        pltpu.make_async_copy(ref, ref, sem).wait()

    def others(axis):
        me = row if axis == "row" else col
        return [lax.rem(me + k, GROUP) for k in (8, 7, 9, 6, 10, 5, 11, 4, 12, 3, 13, 2, 14, 1, 15)]

    def nth(first, i):
        return lax.rem(first + 1 + i, TILES)

    def span(tile):
        return pl.ds(pl.multiple_of(tile * TILE, TILE), TILE)

    def load(i):
        return pltpu.make_async_copy(h_ref.at[span(i), :], h.at[span(i), :], h_sem.at[i])

    barrier = pltpu.get_barrier_semaphore()
    for axis in ("row", "col"):
        for index in others(axis):
            pl.semaphore_signal(
                barrier, inc=1, device_id=peer(axis, index), device_id_type=pl.DeviceIdType.MESH
            )
    for index in others("col"):
        pl.semaphore_signal(
            barrier, inc=1, device_id=(mate_row, index), device_id_type=pl.DeviceIdType.MESH
        )

    fetch = pltpu.make_async_copy(v_ref, v_own, v_sem)
    fetch.start()
    for i in range(TILES):
        load(i).start()

    lane = lax.broadcasted_iota(jnp.int32, (NVEC, TILE), 1)
    fetch.wait()
    start = jnp.concatenate(
        [v_own[:, 0, :], jnp.zeros((NVEC, TILE - PIECE), F32)], axis=1
    )
    v0_own[...] = start
    p0_own[...] = start.astype(BF16)
    sq[0] = jnp.sum(start * start, axis=1, keepdims=True)
    for n in (1, 2, 3):
        sq[n] = jnp.zeros((NVEC, 1), F32)
    pl.semaphore_wait(barrier, 3 * (GROUP - 1))

    for index in others("row"):
        send(p0_own, p0.at[row], p0_s, p0_r, "row", index)
    p0[row] = start.astype(BF16)

    first_tile = (PIECE * row) // TILE
    last_tile = (PIECE * row + PIECE - 1) // TILE
    for n, tile in enumerate((first_tile, last_tile)):
        home = row_home(tile)
        slot = row - (TILE * tile) // PIECE
        wanted = jnp.bool_(True) if n == 0 else last_tile != first_tile

        @pl.when(wanted & (home != row))
        def _():
            send(v0_own, v0_in.at[slot], v0_s.at[n], v0_r.at[slot], "row", home)

        @pl.when(wanted & (home == row))
        def _():
            v0_in[slot] = start

    @pl.loop(0, TILES)
    def _(i):
        load(i).wait()
        for k in range(TILES):
            h_t[k * TILE : (k + 1) * TILE, span(i)] = h[span(i), k * TILE : (k + 1) * TILE].T

    wait_for(p0.at[pl.ds(0, GROUP - 1)], p0_r)
    tiles = [jnp.zeros((NVEC, TILE), F32) for _ in range(TILES)]
    for j in range(GROUP):
        at, shift = divmod(PIECE * j, TILE)
        piece = p0[j].astype(F32)
        turned = pltpu.roll(piece, shift, axis=1) if shift else piece
        tiles[at] = jnp.where((lane >= shift) & (lane < shift + PIECE), turned, tiles[at])
        if shift + PIECE > TILE:
            tiles[at + 1] = jnp.where(lane < shift + PIECE - TILE, turned, tiles[at + 1])
    for k in range(TILES):
        x0[k] = tiles[k].astype(BF16)

    def multiply(x, matrix, first, is_red, axis, part, arrived, n):
        narrow = jnp.concatenate([x[k] for k in range(TILES)], axis=1)

        def hand_over(i, value):
            tile = nth(first, i)
            part[i] = value
            if axis == "row":
                device, place, arrival = (row_home(tile), col), arrived.at[row], rs_r.at[n, 0]
            else:
                device = (odd_row, col_home(tile, parity))
                place, arrival = arrived.at[parity, col], rs_r.at[n, parity]
            send_to(part.at[i], place, rs_s.at[n], arrival, device)

        before = None
        for i in range(TILES):
            value = jnp.dot(
                narrow, matrix[:, span(nth(first, i))], preferred_element_type=F32
            )
            if i:
                hand_over(i - 1, before)
            before = value

        @pl.when(is_red)
        def _():
            if axis == "row":
                arrived[row] = before
            else:
                arrived[1, col] = before

        @pl.when(jnp.logical_not(is_red))
        def _():
            hand_over(TILES - 1, before)

    def summed(arrived, n, group, count):
        wait_for(arrived.at[pl.ds(0, count)], rs_r.at[n, group])
        terms = [arrived[j] for j in range(GROUP)]
        while len(terms) > 1:
            terms = [terms[k] + terms[k + 1] for k in range(0, len(terms), 2)]
        return terms[0]

    def to_all(value, own, dest, tile, s_sem, r_sem, devices, mine):
        own[...] = value.astype(BF16)
        for device in devices:
            send_to(own, dest.at[tile], s_sem, r_sem, device)
        if mine:
            dest[tile] = value.astype(BF16)

    def gathered(dest, is_red, n):
        @pl.when(is_red)
        def _():
            wait_for(dest.at[pl.ds(0, TILES - 1)], ag_r.at[n])

        @pl.when(jnp.logical_not(is_red))
        def _():
            wait_for(dest, ag_r.at[n])

    def square(value):
        return jnp.sum(value * value, axis=1, keepdims=True)

    multiply(x0, h_t, col_tile, col_red, "col", part1, in1, 0)

    for group in (0, 1):

        @pl.when(col_reds[group])
        def _():
            v1 = summed(in1.at[group], 0, group, GROUP - group)
            devices = [(row - 1 + group, index) for index in others("col")]
            if group == 0:
                devices.append((row - 1, col))
            to_all(
                v1, ag1_own.at[group], ag1, col_tiles[group],
                ag_s.at[group], ag_r.at[0], devices, group == 1,
            )
            v1_keep[group] = v1
            sq[1] += square(v1)

    gathered(ag1, col_red, 0)

    multiply(ag1, h, row_tile, row_red, "row", part2, in2, 1)

    @pl.when(row_red)
    def _():
        v0 = jnp.zeros((NVEC, TILE), F32)
        for slot in range(3):
            owner = (TILE * row_tile) // PIECE + slot
            offset = PIECE * owner - TILE * row_tile

            @pl.when((offset < TILE) & (owner != row))
            def _():
                wait_for(v0_in.at[slot], v0_r.at[slot])

            turned = pltpu.roll(v0_in[slot], lax.rem(offset + TILE, TILE), axis=1)
            v0 = jnp.where((lane >= offset) & (lane < offset + PIECE), turned, v0)
        v2 = 2.0 * summed(in2, 1, 0, GROUP - 1) - v0
        devices = [(index, col) for index in others("row")]
        to_all(v2, ag2_own, ag2, row_tile, ag_s.at[2], ag_r.at[1], devices, True)
        sq[2] = square(v2)

    gathered(ag2, row_red, 1)

    multiply(ag2, h_t, col_tile, col_red, "col", part3, in3, 2)

    def out_dest(group, slot):
        tile = col_tiles[group]
        owner = (TILE * tile) // PIECE + slot
        wanted = col_reds[group] & (PIECE * owner < TILE * (tile + 1))
        return owner, wanted, tile - (PIECE * owner) // TILE

    for group in (0, 1):

        @pl.when(col_reds[group])
        def _():
            v3 = 2.0 * summed(in3.at[group], 2, group, GROUP - group) - v1_keep[group]
            out_own[group] = v3
            sq[3] += square(v3)

    wide = lax.broadcasted_iota(jnp.int32, (NVEC, 128), 1)
    sub = lax.broadcasted_iota(jnp.int32, (NVEC, 128), 0)
    packed = jnp.zeros((NVEC, 128), F32)
    for n in range(4):
        packed = jnp.where(wide == 4 * sub + n, sq[n], packed)

    def everywhere(value, own, dest, axis, n):
        me = row if axis == "row" else col
        own[...] = value
        for index in others(axis):
            send(own, dest.at[me], m_s.at[n], m_r.at[n], axis, index)
        dest[me] = value

    def total(dest, n):
        wait_for(dest.at[pl.ds(0, GROUP - 1)], m_r.at[n])
        terms = [dest[j] for j in range(GROUP)]
        while len(terms) > 1:
            terms = [terms[k] + terms[k + 1] for k in range(0, len(terms), 2)]
        return terms[0]

    everywhere(jnp.sum(packed, axis=0, keepdims=True), m1_own, m1, "col", 0)

    for group in (0, 1):
        for slot in range(3):
            owner, wanted, place = out_dest(group, slot)
            mine = (owner == col) if group else jnp.bool_(False)

            @pl.when(wanted & jnp.logical_not(mine))
            def _():
                send_to(
                    out_own.at[group], out_in.at[place], out_s.at[group, slot], out_r.at[place],
                    (row - 1 + group, owner),
                )

            if group:

                @pl.when(wanted & mine)
                def _():
                    out_in[place] = out_own[group]

    everywhere(total(m1, 0), m2_own, m2, "row", 1)

    from_tile = (PIECE * col) // TILE
    upto_tile = (PIECE * col + PIECE - 1) // TILE

    def elsewhere(tile):
        return (parity == 0) | (col_home(tile, parity) != col)

    @pl.when(elsewhere(from_tile))
    def _():
        wait_for(out_in.at[0], out_r.at[0])

    @pl.when((upto_tile != from_tile) & elsewhere(upto_tile))
    def _():
        wait_for(out_in.at[1], out_r.at[1])

    both = jnp.concatenate([out_in[0], out_in[1]], axis=1)
    begin = PIECE * col - TILE * from_tile
    last_ref[...] = pltpu.roll(both, lax.rem(2 * TILE - begin, 2 * TILE), axis=1)[:, :PIECE]

    wait_for(p0.at[pl.ds(0, GROUP - 1)], p0_s)
    for n, tile in enumerate((first_tile, last_tile)):
        wanted = jnp.bool_(True) if n == 0 else last_tile != first_tile

        @pl.when(wanted & (row_home(tile) != row))
        def _():
            wait_for(v0_own, v0_s.at[n])

    for n, (part, is_red) in enumerate(((part1, col_red), (part2, row_red), (part3, col_red))):

        @pl.when(is_red)
        def _():
            wait_for(part.at[pl.ds(0, TILES - 1)], rs_s.at[n])

        @pl.when(jnp.logical_not(is_red))
        def _():
            wait_for(part, rs_s.at[n])

    for n, is_red in enumerate((*col_reds, row_red)):

        @pl.when(is_red)
        def _():
            wait_for(p0.at[pl.ds(0, GROUP if n == 0 else GROUP - 1)], ag_s.at[n])

    for group in (0, 1):
        for slot in range(3):
            owner, wanted, _place = out_dest(group, slot)
            mine = (owner == col) if group else jnp.bool_(False)

            @pl.when(wanted & jnp.logical_not(mine))
            def _():
                wait_for(out_own.at[group], out_s.at[group, slot])

    wait_for(m1.at[pl.ds(0, GROUP - 1)], m_s.at[0])

    squares = total(m2, 1) / ORDER
    spread = jnp.broadcast_to(squares, (NVEC, 128))
    by_order = [
        jnp.sum(jnp.where(wide == 4 * sub + n, spread, 0.0), axis=1, keepdims=True)
        for n in range(4)
    ]
    mom_ref[...] = jnp.concatenate(
        [by_order[0]] + [2.0 * by_order[n] - by_order[0] for n in (1, 2, 3)], axis=1
    )
    wait_for(m2.at[pl.ds(0, GROUP - 1)], m_s.at[1])


def per_device(hamiltonian, start_vectors):
    dma = pltpu.SemaphoreType.DMA
    rowed = pltpu.VMEM((GROUP, 1, 128), F32)
    tile = pltpu.VMEM((NVEC, TILE), F32)
    narrow = pltpu.VMEM((NVEC, TILE), BF16)
    return pl.pallas_call(
        kernel,
        out_shape=(
            pltpu.VMEM((NVEC, PIECE), F32),
            pltpu.VMEM((NVEC, 4), F32),
        ),
        in_specs=[
            pl.BlockSpec(memory_space=pl.ANY),
            pl.BlockSpec(memory_space=pl.ANY),
        ],
        out_specs=(
            pl.BlockSpec(memory_space=pltpu.VMEM),
            pl.BlockSpec(memory_space=pltpu.VMEM),
        ),
        scratch_shapes=[
            pltpu.VMEM((NVEC, 1, PIECE), F32),
            pltpu.VMEM((BLOCK, BLOCK), BF16),
            pltpu.VMEM((BLOCK, BLOCK), BF16),
            narrow, pltpu.VMEM((GROUP, NVEC, TILE), BF16),
            tile, pltpu.VMEM((3, NVEC, TILE), F32),
            pltpu.VMEM((TILES, NVEC, TILE), BF16), pltpu.VMEM((2, NVEC, TILE), F32),
            pltpu.VMEM((TILES, NVEC, TILE), F32), pltpu.VMEM((2, GROUP, NVEC, TILE), F32),
            pltpu.VMEM((2, NVEC, TILE), BF16), pltpu.VMEM((TILES, NVEC, TILE), BF16),
            pltpu.VMEM((TILES, NVEC, TILE), F32), pltpu.VMEM((GROUP, NVEC, TILE), F32),
            narrow, pltpu.VMEM((TILES, NVEC, TILE), BF16),
            pltpu.VMEM((TILES, NVEC, TILE), F32), pltpu.VMEM((2, GROUP, NVEC, TILE), F32),
            pltpu.VMEM((2, NVEC, TILE), F32), pltpu.VMEM((2, NVEC, TILE), F32),
            pltpu.VMEM((4, NVEC, 1), F32),
            pltpu.VMEM((1, 128), F32), rowed, pltpu.VMEM((1, 128), F32), rowed,
            dma(()), dma((TILES,)), dma(()), dma(()), dma((2,)), dma((3,)), dma((3,)),
            dma((3, 2)), dma((3,)), dma((2,)), dma((2, 3)), dma((2,)), dma((2,)), dma((2,)),
        ],
        compiler_params=pltpu.CompilerParams(
            collective_id=0, has_side_effects=True, vmem_limit_bytes=60 * 1024 * 1024
        ),
    )(hamiltonian, start_vectors)


def solution(mesh):
    return jax.shard_map(
        per_device,
        mesh=mesh,
        in_specs=(P("row", "col"), P(None, "col", "row")),
        out_specs=(P(None, ("row", "col")), P()),
        check_vma=False,
    )
```

```python
import functools

import jax
import jax.numpy as jnp
from jax import lax
from jax.experimental import pallas as pl
from jax.experimental.pallas import tpu as pltpu
from jax.sharding import PartitionSpec as P

ORDER = 36864
NVEC = 8
GROUP = 16
PIECE = 144
TILE = 256
TILES = 9
BLOCK = TILE * TILES
F32 = jnp.float32
BF16 = jnp.bfloat16


def row_home(tile):
    return jnp.where(tile == TILES - 1, 8, 2 * tile + 1)


def col_home(tile, parity):
    return jnp.where(parity == 0, tile, GROUP - 1 - tile)


def kernel(
    h_ref, v_ref, last_ref, mom_ref,
    v_own, h, h_t, p0_own, p0, v0_own, v0_in, x0, v1_keep,
    part1, in1, ag1_own, ag1, part2, in2, ag2_own, ag2, part3, in3,
    sofar, out_own, out_in, sq, m1_own, m1, m2_own, m2,
    v_sem, h_sem, p0_s, p0_r, v0_s, v0_r, rs_s, rs_r, ag_s, ag_r, out_s, out_r, m_s, m_r,
):
    row, col = lax.axis_index("row"), lax.axis_index("col")
    parity = lax.rem(row, 2)

    chip = row // 2
    row_red = (parity == 1) | (row == 8)
    row_tile = jnp.where(row == 8, TILES - 1, chip)
    col_tiles = (col, GROUP - 1 - col)
    col_reds = tuple((parity == 1) & (tile < TILES) for tile in col_tiles)
    col_red = col_reds[1]
    col_slot = jnp.where(parity == 0, col, GROUP - 1 - col)
    col_tile = jnp.where(col_slot < TILES, col_slot, col_slot - 7)
    odd_row = row + 1 - parity
    mate_row = row + 1 - 2 * parity

    def peer(axis, index):
        return (index, col) if axis == "row" else (row, index)

    def send_to(src, dst, s_sem, r_sem, device):
        pltpu.make_async_remote_copy(
            src_ref=src, dst_ref=dst, send_sem=s_sem, recv_sem=r_sem,
            device_id=device, device_id_type=pl.DeviceIdType.MESH,
        ).start()

    def send(src, dst, s_sem, r_sem, axis, index):
        send_to(src, dst, s_sem, r_sem, peer(axis, index))

    def wait_for(ref, sem):
        pltpu.make_async_copy(ref, ref, sem).wait()

    def others(axis):
        if axis == "row":
            return [lax.rem(row + k, GROUP) for k in (8, 7, 9, 6, 10, 5, 11, 4, 12, 3, 13, 2, 14, 1, 15)]
        steps = [(dx, dy) for dx in range(4) for dy in range(4) if dx or dy]
        steps.sort(key=lambda s: -min(s[0], 4 - s[0]) - min(s[1], 4 - s[1]))
        return [
            lax.rem(col // 4 + dx, 4) * 4 + lax.rem(lax.rem(col, 4) + dy, 4) for dx, dy in steps
        ]

    def nth(first, i):
        return lax.rem(first + 1 + i, TILES)

    def span(tile):
        return pl.ds(pl.multiple_of(tile * TILE, TILE), TILE)

    def load(i):
        return pltpu.make_async_copy(h_ref.at[span(i), :], h.at[span(i), :], h_sem.at[i])

    barrier = pltpu.get_barrier_semaphore()
    for axis in ("row", "col"):
        for index in others(axis):
            pl.semaphore_signal(
                barrier, inc=1, device_id=peer(axis, index), device_id_type=pl.DeviceIdType.MESH
            )
    for index in others("col"):
        pl.semaphore_signal(
            barrier, inc=1, device_id=(mate_row, index), device_id_type=pl.DeviceIdType.MESH
        )

    fetch = pltpu.make_async_copy(v_ref, v_own, v_sem)
    fetch.start()
    for i in range(TILES):
        load(i).start()

    lane = lax.broadcasted_iota(jnp.int32, (NVEC, TILE), 1)
    fetch.wait()
    start = jnp.concatenate(
        [v_own[:, 0, :], jnp.zeros((NVEC, TILE - PIECE), F32)], axis=1
    )
    v0_own[...] = start
    p0_own[...] = start.astype(BF16)
    sq[0] = jnp.sum(start * start, axis=1, keepdims=True)
    for n in (1, 2, 3):
        sq[n] = jnp.zeros((NVEC, 1), F32)
    pl.semaphore_wait(barrier, 3 * (GROUP - 1))

    for index in others("row"):
        send(p0_own, p0.at[row], p0_s, p0_r, "row", index)
    p0[row] = start.astype(BF16)

    @pl.loop(0, TILES)
    def _(i):
        load(i).wait()
        for k in range(TILES):
            h_t[k * TILE : (k + 1) * TILE, span(i)] = h[span(i), k * TILE : (k + 1) * TILE].T

    wait_for(p0.at[pl.ds(0, GROUP - 1)], p0_r)
    tiles = [jnp.zeros((NVEC, TILE), F32) for _ in range(TILES)]
    for j in range(GROUP):
        at, shift = divmod(PIECE * j, TILE)
        piece = p0[j].astype(F32)
        turned = pltpu.roll(piece, shift, axis=1) if shift else piece
        tiles[at] = jnp.where((lane >= shift) & (lane < shift + PIECE), turned, tiles[at])
        if shift + PIECE > TILE:
            tiles[at + 1] = jnp.where(lane < shift + PIECE - TILE, turned, tiles[at + 1])
    for k in range(TILES):
        x0[k] = tiles[k].astype(BF16)

    def multiply(x, matrix, first, is_red, axis, part, arrived, n, arrive, early, late):
        def product(tiles, columns):
            return sum(
                jnp.dot(x[k], matrix[span(k), columns], preferred_element_type=F32)
                for k in tiles
            )

        if early:
            for k in early:
                arrive(k)
            for i in range(TILES):
                sofar[i] = product(early, slice(i * TILE, (i + 1) * TILE))
            for k in late:
                arrive(k)

        def hand_over(i, value):
            tile = nth(first, i)
            part[i] = value
            if axis == "row":
                device, place, arrival = (row_home(tile), col), arrived.at[row], rs_r.at[n, 0]
            else:
                device = (odd_row, col_home(tile, parity))
                place, arrival = arrived.at[parity, col], rs_r.at[n, parity]
            send_to(part.at[i], place, rs_s.at[n], arrival, device)

        before = None
        for i in range(TILES):
            tile = nth(first, i)
            value = product(late, span(tile))
            if early:
                value = value + sofar[tile]
            if i:
                hand_over(i - 1, before)
            before = value

        @pl.when(is_red)
        def _():
            if axis == "row":
                arrived[row] = before
            else:
                arrived[1, col] = before

        @pl.when(jnp.logical_not(is_red))
        def _():
            hand_over(TILES - 1, before)

    def summed(arrived, n, group, count):
        wait_for(arrived.at[pl.ds(0, count)], rs_r.at[n, group])
        terms = [arrived[j] for j in range(GROUP)]
        while len(terms) > 1:
            terms = [terms[k] + terms[k + 1] for k in range(0, len(terms), 2)]
        return terms[0]

    def to_all(value, own, dest, tile, s_sem, r_sem, devices, mine):
        own[...] = value.astype(BF16)
        for device in devices:
            send_to(own, dest.at[tile], s_sem, r_sem, device)
        if mine:
            dest[tile] = value.astype(BF16)

    def gathered(dest, is_red, own, n):
        def arrive(tile):
            @pl.when(jnp.logical_not(is_red & (own == tile)))
            def _():
                wait_for(dest.at[tile], ag_r.at[n, tile])

        return arrive

    def square(value):
        return jnp.sum(value * value, axis=1, keepdims=True)

    multiply(x0, h_t, col_tile, col_red, "col", part1, in1, 0, None, (), tuple(range(TILES)))

    first_tile = (PIECE * row) // TILE
    last_tile = (PIECE * row + PIECE - 1) // TILE
    for n, tile in enumerate((first_tile, last_tile)):
        home = row_home(tile)
        slot = row - (TILE * tile) // PIECE
        wanted = jnp.bool_(True) if n == 0 else last_tile != first_tile

        @pl.when(wanted & (home != row))
        def _():
            send(v0_own, v0_in.at[slot], v0_s.at[n], v0_r.at[slot], "row", home)

        @pl.when(wanted & (home == row))
        def _():
            v0_in[slot] = start

    for group in (0, 1):

        @pl.when(col_reds[group])
        def _():
            v1 = summed(in1.at[group], 0, group, GROUP - group)
            devices = [(row - 1 + group, index) for index in others("col")]
            if group == 0:
                devices.append((row - 1, col))
            to_all(
                v1, ag1_own.at[group], ag1, col_tiles[group],
                ag_s.at[group], ag_r.at[0, col_tiles[group]], devices, group == 1,
            )
            v1_keep[group] = v1
            sq[1] += square(v1)

    across = jnp.where(parity == 0, col // 4, 3 - col // 4)
    base = jnp.where((across == 1) | (across == 2), 4, 0)
    near = [base + k for k in range(4)]
    far = [4 - base + k for k in range(4)] + [8]
    arrive = gathered(ag1, col_red, col_tiles[1], 0)

    multiply(ag1, h, row_tile, row_red, "row", part2, in2, 1, arrive, near, far)

    @pl.when(row_red)
    def _():
        v0 = jnp.zeros((NVEC, TILE), F32)
        for slot in range(3):
            owner = (TILE * row_tile) // PIECE + slot
            offset = PIECE * owner - TILE * row_tile

            @pl.when((offset < TILE) & (owner != row))
            def _():
                wait_for(v0_in.at[slot], v0_r.at[slot])

            turned = pltpu.roll(v0_in[slot], lax.rem(offset + TILE, TILE), axis=1)
            v0 = jnp.where((lane >= offset) & (lane < offset + PIECE), turned, v0)
        v2 = 2.0 * summed(in2, 1, 0, GROUP - 1) - v0
        devices = [(index, col) for index in others("row")]
        to_all(v2, ag2_own, ag2, row_tile, ag_s.at[2], ag_r.at[1, row_tile], devices, True)
        sq[2] = square(v2)

    near = [lax.rem(chip + k, 8) for k in (0, 1, 7, 2, 6)]
    far = [lax.rem(chip + k, 8) for k in (3, 5, 4)] + [8]
    arrive = gathered(ag2, row_red, row_tile, 1)

    multiply(ag2, h_t, col_tile, col_red, "col", part3, in3, 2, arrive, near, far)

    def out_dest(group, slot):
        tile = col_tiles[group]
        owner = (TILE * tile) // PIECE + slot
        wanted = col_reds[group] & (PIECE * owner < TILE * (tile + 1))
        return owner, wanted, tile - (PIECE * owner) // TILE

    for group in (0, 1):

        @pl.when(col_reds[group])
        def _():
            v3 = 2.0 * summed(in3.at[group], 2, group, GROUP - group) - v1_keep[group]
            out_own[group] = v3
            sq[3] += square(v3)

    wide = lax.broadcasted_iota(jnp.int32, (NVEC, 128), 1)
    sub = lax.broadcasted_iota(jnp.int32, (NVEC, 128), 0)
    packed = jnp.zeros((NVEC, 128), F32)
    for n in range(4):
        packed = jnp.where(wide == 4 * sub + n, sq[n], packed)

    def everywhere(value, own, dest, axis, n):
        me = row if axis == "row" else col
        own[...] = value
        for index in others(axis):
            send(own, dest.at[me], m_s.at[n], m_r.at[n], axis, index)
        dest[me] = value

    def total(dest, n):
        wait_for(dest.at[pl.ds(0, GROUP - 1)], m_r.at[n])
        terms = [dest[j] for j in range(GROUP)]
        while len(terms) > 1:
            terms = [terms[k] + terms[k + 1] for k in range(0, len(terms), 2)]
        return terms[0]

    everywhere(jnp.sum(packed, axis=0, keepdims=True), m1_own, m1, "col", 0)

    for group in (0, 1):
        for slot in range(3):
            owner, wanted, place = out_dest(group, slot)
            mine = (owner == col) if group else jnp.bool_(False)

            @pl.when(wanted & jnp.logical_not(mine))
            def _():
                send_to(
                    out_own.at[group], out_in.at[place], out_s.at[group, slot], out_r.at[place],
                    (row - 1 + group, owner),
                )

            if group:

                @pl.when(wanted & mine)
                def _():
                    out_in[place] = out_own[group]

    everywhere(total(m1, 0), m2_own, m2, "row", 1)

    from_tile = (PIECE * col) // TILE
    upto_tile = (PIECE * col + PIECE - 1) // TILE

    def elsewhere(tile):
        return (parity == 0) | (col_home(tile, parity) != col)

    @pl.when(elsewhere(from_tile))
    def _():
        wait_for(out_in.at[0], out_r.at[0])

    @pl.when((upto_tile != from_tile) & elsewhere(upto_tile))
    def _():
        wait_for(out_in.at[1], out_r.at[1])

    both = jnp.concatenate([out_in[0], out_in[1]], axis=1)
    begin = PIECE * col - TILE * from_tile
    last_ref[...] = pltpu.roll(both, lax.rem(2 * TILE - begin, 2 * TILE), axis=1)[:, :PIECE]

    wait_for(p0.at[pl.ds(0, GROUP - 1)], p0_s)
    for n, tile in enumerate((first_tile, last_tile)):
        wanted = jnp.bool_(True) if n == 0 else last_tile != first_tile

        @pl.when(wanted & (row_home(tile) != row))
        def _():
            wait_for(v0_own, v0_s.at[n])

    for n, (part, is_red) in enumerate(((part1, col_red), (part2, row_red), (part3, col_red))):

        @pl.when(is_red)
        def _():
            wait_for(part.at[pl.ds(0, TILES - 1)], rs_s.at[n])

        @pl.when(jnp.logical_not(is_red))
        def _():
            wait_for(part, rs_s.at[n])

    for n, is_red in enumerate((*col_reds, row_red)):

        @pl.when(is_red)
        def _():
            wait_for(p0.at[pl.ds(0, GROUP if n == 0 else GROUP - 1)], ag_s.at[n])

    for group in (0, 1):
        for slot in range(3):
            owner, wanted, _place = out_dest(group, slot)
            mine = (owner == col) if group else jnp.bool_(False)

            @pl.when(wanted & jnp.logical_not(mine))
            def _():
                wait_for(out_own.at[group], out_s.at[group, slot])

    wait_for(m1.at[pl.ds(0, GROUP - 1)], m_s.at[0])

    squares = total(m2, 1) / ORDER
    spread = jnp.broadcast_to(squares, (NVEC, 128))
    by_order = [
        jnp.sum(jnp.where(wide == 4 * sub + n, spread, 0.0), axis=1, keepdims=True)
        for n in range(4)
    ]
    mom_ref[...] = jnp.concatenate(
        [by_order[0]] + [2.0 * by_order[n] - by_order[0] for n in (1, 2, 3)], axis=1
    )
    wait_for(m2.at[pl.ds(0, GROUP - 1)], m_s.at[1])


def per_device(hamiltonian, start_vectors):
    dma = pltpu.SemaphoreType.DMA
    rowed = pltpu.VMEM((GROUP, 1, 128), F32)
    tile = pltpu.VMEM((NVEC, TILE), F32)
    narrow = pltpu.VMEM((NVEC, TILE), BF16)
    return pl.pallas_call(
        kernel,
        out_shape=(
            pltpu.VMEM((NVEC, PIECE), F32),
            pltpu.VMEM((NVEC, 4), F32),
        ),
        in_specs=[
            pl.BlockSpec(memory_space=pl.ANY),
            pl.BlockSpec(memory_space=pl.ANY),
        ],
        out_specs=(
            pl.BlockSpec(memory_space=pltpu.VMEM),
            pl.BlockSpec(memory_space=pltpu.VMEM),
        ),
        scratch_shapes=[
            pltpu.VMEM((NVEC, 1, PIECE), F32),
            pltpu.VMEM((BLOCK, BLOCK), BF16),
            pltpu.VMEM((BLOCK, BLOCK), BF16),
            narrow, pltpu.VMEM((GROUP, NVEC, TILE), BF16),
            tile, pltpu.VMEM((3, NVEC, TILE), F32),
            pltpu.VMEM((TILES, NVEC, TILE), BF16), pltpu.VMEM((2, NVEC, TILE), F32),
            pltpu.VMEM((TILES, NVEC, TILE), F32), pltpu.VMEM((2, GROUP, NVEC, TILE), F32),
            pltpu.VMEM((2, NVEC, TILE), BF16), pltpu.VMEM((TILES, NVEC, TILE), BF16),
            pltpu.VMEM((TILES, NVEC, TILE), F32), pltpu.VMEM((GROUP, NVEC, TILE), F32),
            narrow, pltpu.VMEM((TILES, NVEC, TILE), BF16),
            pltpu.VMEM((TILES, NVEC, TILE), F32), pltpu.VMEM((2, GROUP, NVEC, TILE), F32),
            pltpu.VMEM((TILES, NVEC, TILE), F32),
            pltpu.VMEM((2, NVEC, TILE), F32), pltpu.VMEM((2, NVEC, TILE), F32),
            pltpu.VMEM((4, NVEC, 1), F32),
            pltpu.VMEM((1, 128), F32), rowed, pltpu.VMEM((1, 128), F32), rowed,
            dma(()), dma((TILES,)), dma(()), dma(()), dma((2,)), dma((3,)), dma((3,)),
            dma((3, 2)), dma((3,)), dma((2, TILES)), dma((2, 3)), dma((2,)), dma((2,)), dma((2,)),
        ],
        compiler_params=pltpu.CompilerParams(
            collective_id=0, has_side_effects=True, vmem_limit_bytes=60 * 1024 * 1024
        ),
    )(hamiltonian, start_vectors)


def solution(mesh):
    return jax.shard_map(
        per_device,
        mesh=mesh,
        in_specs=(P("row", "col"), P(None, "col", "row")),
        out_specs=(P(None, ("row", "col")), P()),
        check_vma=False,
    )
```
